256 devices in a mesh: rows: 16 (over z, core), cols: 16 (over y, x).
Axes of the slice: x: 4, y: 4, z: 8, core: 2. Of those that a mesh axis runs over, the one named last changes fastest.
Arguments:
- solved_bases: float32 [6, 128, 131072], P(None, 'cols', 'rows'), may hold values from -6 to 6
- right_bases: float32 [5, 128, 131072], P(None, 'cols', 'rows'), may hold values from -1 to 1, as said below
Outputs:
- factored_bases: float32 [5, 128, 131072], P(None, 'cols', 'rows')
The draws below stay inside these ranges and needn't reach their ends.
Inputs may be any that keep to these rules, and one draw needn't show every extreme that they name: `right_bases`: level l is drawn with a deviation of 0.025 / sqrt(2048 * 2**l).
All inputs are finite; a program needn't handle non-finite values.
Results may differ from the reference program's by a relative error of at most 0.0001.
Values sent between devices are 32-bit elements; how exact they have to be, the bound alone decides.
No kernel may reach another device: no remote copies, remote signals or barrier semaphores. Data moves between devices by JAX's collectives and lax.ppermute only.
A program may use at most 128 MiB of HBM per device.

```python
import jax
import jax.numpy as jnp
from jax import lax

K = 128
LEVELS = 6
NTOT = 131072
LEAF = 2048


def draw_right_bases(key, part):
    level_ids = jnp.arange(LEVELS - 1).astype(jnp.float32)
    node_rows = LEAF * jnp.exp2(level_ids)
    scales = 0.025 / jnp.sqrt(node_rows)
    base = jnp.clip(jax.random.normal(key, (LEVELS - 1, K, NTOT), jnp.float32), -6.0, 6.0)
    return base * scales[:, None, None]


def steps_of(key, extent, pieces, least, high):
    level, own = 1.0, jax.random.fold_in(key, 6)
    for axis_at, blocks in pieces:
        heights = jnp.exp(jax.random.uniform(jax.random.fold_in(own, axis_at), (blocks,), jnp.float32, least / len(pieces), high / len(pieces)))
        level = level * jnp.repeat(heights, extent[axis_at] // blocks).reshape([-1 if axis == axis_at else 1 for axis in range(len(extent))])
    return level


def centred(stream_key, shape, width, most, shards=(), kind=jnp.bfloat16):
    level = steps_of(stream_key, shape, shards, -0.22, 0.18) if shards else 1.0
    drawn = jax.random.normal(stream_key, shape, jnp.float32) * width * level
    return jnp.minimum(jnp.maximum(drawn, -most), most).astype(kind)


def setup_inputs(seed: int = 0) -> dict:
    streams_of = jax.random.split(jax.random.key(seed), 3)
    solved_bases = centred(streams_of[0], (LEVELS, K, NTOT), 1.0, 6.0, ((1, 16), (2, 16)), jnp.float32)
    right_bases = draw_right_bases(jax.random.fold_in(streams_of[2], 71), 0)
    return dict(solved_bases=solved_bases, right_bases=right_bases)


def reference(solved_bases, right_bases):
    highest = lax.Precision.HIGHEST
    bases = [solved_bases[member] for member in range(LEVELS)]
    identity = jnp.eye(K, dtype=jnp.float32)
    for this_level in range(LEVELS - 1):
        node_rows = LEAF * 2 ** this_level
        parents = NTOT // (2 * node_rows)
        right = right_bases[this_level].reshape(K, parents, 2, node_rows)
        solved = bases[this_level].reshape(K, parents, 2, node_rows)
        coupling = jnp.einsum('apcr,bpcr->pcab', right, solved, precision=highest)
        identities = jnp.broadcast_to(identity, (parents, K, K))
        system = jnp.concatenate([jnp.concatenate([identities, coupling[:, 1]], 2), jnp.concatenate([coupling[:, 0], identities], 2)], 1)
        for member in range(this_level + 1, LEVELS):
            coarse = bases[member].reshape(K, parents, 2, node_rows)
            projected = jnp.einsum('apcr,bpcr->pcab', right, coarse, precision=highest)
            right_sides = jnp.concatenate([projected[:, 1], projected[:, 0]], 1)
            solution = jnp.linalg.solve(system, right_sides).reshape(parents, 2, K, K)
            update = jnp.einsum('pcab,apcr->bpcr', solution, solved, precision=highest)
            bases[member] = (coarse - update).reshape(K, NTOT)
    return jnp.stack(bases[1:])
```

```python
import functools

import jax
import jax.numpy as jnp
import numpy as np
from jax import lax
from jax.experimental import pallas as pl
from jax.experimental.pallas import tpu as pltpu
from jax.sharding import Mesh
from jax.sharding import PartitionSpec as P

ROWS = ("zt", "z1", "z0", "core")
COLS = ("yh", "yl", "x")
GROUP = ("yl", "x")
LEVELS = 6
K = 128
HIGHEST = lax.Precision.HIGHEST


def dot(a, b):
    return jnp.dot(a, b, precision=HIGHEST, preferred_element_type=jnp.float32)


def dot_t(a, b):
    return lax.dot_general(a, b, (((1,), (1,)), ((), ())), precision=HIGHEST, preferred_element_type=jnp.float32)


def inverse(coupling, x_ref, r_ref):
    rows = lax.broadcasted_iota(jnp.int32, (K, K), 0)
    cols = lax.broadcasted_iota(jnp.int32, (K, K), 1)
    eye = jnp.where(rows == cols, 1.0, 0.0).astype(jnp.float32)
    matrix = eye - coupling
    square = dot(coupling, coupling)
    quick = jnp.sum(square * square) < 0.25

    @pl.when(quick)
    def _():
        x_ref[...] = eye + coupling
        r_ref[...] = square

    @pl.when(jnp.logical_not(quick))
    def _():
        size = jnp.abs(matrix)
        scale = 1.0 / (jnp.max(jnp.sum(size, axis=0)) * jnp.max(jnp.sum(size, axis=1)))
        start = matrix.T * scale
        x_ref[...] = start
        r_ref[...] = eye - dot(start, matrix)

    def size_of(r):
        return jnp.sum(r * r)

    def going(carry):
        step, size = carry
        return jnp.logical_and(step < 80, size > 1e-6)

    def refine(carry):
        step, _ = carry
        x = x_ref[...] + dot(r_ref[...], x_ref[...])
        r = eye - dot(x, matrix)
        x_ref[...] = x
        r_ref[...] = r
        return step + 1, size_of(r)

    lax.while_loop(going, refine, (jnp.int32(0), size_of(r_ref[...])))
    x_ref[...] = x_ref[...] + dot(r_ref[...], x_ref[...])


def eliminate(panel1, panel2, rest1, rest2, x_ref, r_ref):
    p1, p2 = panel1[:, :K], panel2[:, :K]
    inverse(dot(p1, p2), x_ref, r_ref)
    q1, q2 = rest1[:, :K], rest2[:, :K]
    x1 = dot(q2 - dot(q1, p2), x_ref[...])
    x2 = q1 - dot(x1, p1)
    if panel1.shape[1] == K:
        return x1, x2, None
    state = rest1[:, K:] + rest2[:, K:] - dot(x1, panel1[:, K:]) - dot(x2, panel2[:, K:])
    return x1, x2, state


def gram_kernel(a_ref, g_ref):
    right = a_ref[:, LEVELS:]
    right = jnp.transpose(right, (1, 0, 2, 3)).reshape((LEVELS - 1) * K, -1)
    for m in range(LEVELS):
        g = dot_t(a_ref[:, m].reshape(K, -1), right)
        g_ref[:, m] = g.reshape(8, 16, (LEVELS - 1) * K)


def level0_kernel(ag_ref, h_ref, x_out, s_out, x_ref, r_ref):
    width = (LEVELS - 1) * K
    p1, p2 = ag_ref[:, 0].reshape(K, width), ag_ref[:, 1].reshape(K, width)
    n = LEVELS - 1
    x1, x2, state = eliminate(
        p1, p2, h_ref[0, 1:].reshape(n * 16, width), h_ref[1, 1:].reshape(n * 16, width), x_ref, r_ref
    )
    x_out[0] = x1.reshape(n, 16, K)
    x_out[1] = x2.reshape(n, 16, K)
    s_out[...] = state.reshape(n, 16, width - K)


def level1_kernel(side_ref, ag_ref, own_ref, other_ref, x_out, s_out, x_ref, r_ref):
    width = (LEVELS - 2) * K
    n = LEVELS - 2
    side = side_ref[0]
    p1 = ag_ref[pl.ds(side * 8, 8)].reshape(K, width)
    p2 = ag_ref[pl.ds((1 - side) * 8, 8)].reshape(K, width)
    x1, _, state = eliminate(
        p1, p2, own_ref[1:].reshape(n * 16, width), other_ref[...].reshape(n * 16, width), x_ref, r_ref
    )
    x_out[...] = x1.reshape(n, 16, K)
    s_out[...] = state.reshape(n, 16, width - K)


def level2_kernel(own_ref, other_ref, x_out, s_out, x_ref, r_ref):
    width = (LEVELS - 3) * K
    n = LEVELS - 3

    def rest(ref):
        return jnp.concatenate([ref[:, m].reshape(K, width) for m in range(1, n + 1)], axis=0)

    x1, _, state = eliminate(
        own_ref[:, 0].reshape(K, width), other_ref[:, 0].reshape(K, width), rest(own_ref), rest(other_ref), x_ref, r_ref
    )
    x_out[...] = x1
    s_out[...] = state


def level3_kernel(own_ref, other_ref, x_out, s_out, x_ref, r_ref):
    x1, _, state = eliminate(own_ref[:K], other_ref[:K], own_ref[K:], other_ref[K:], x_ref, r_ref)
    x_out[...] = x1
    s_out[...] = state


def level4_kernel(own_ref, other_ref, x_out, x_ref, r_ref):
    x1, _, _ = eliminate(own_ref[:K], other_ref[:K], own_ref[K:], other_ref[K:], x_ref, r_ref)
    x_out[...] = x1


def finish_kernel(a_ref, x0_ref, x1_ref, x2_ref, x3_ref, x4_ref, o_ref):
    done = [a_ref[:, 0].reshape(K, -1)]

    def factor(level, i):
        if level == 0:
            return x0_ref[:, i].reshape(K, K)
        if level == 1:
            return x1_ref[:, i].reshape(K, K)
        return (x2_ref, x3_ref, x4_ref)[level - 2][i * K : (i + 1) * K]

    for m in range(1, LEVELS):
        value = a_ref[:, m].reshape(K, -1)
        for level in range(m):
            value = value - dot(factor(level, m - level - 1), done[level])
        done.append(value)
        o_ref[:, m - 1] = value.reshape(16, 8, -1)


def call(kernel, outs, *args, scalar=False, flops=10**8):
    vmem = pl.BlockSpec(memory_space=pltpu.VMEM)
    specs = [vmem] * len(args)
    if scalar:
        specs[0] = pl.BlockSpec(memory_space=pltpu.SMEM)
    scratch = []
    if kernel not in (gram_kernel, finish_kernel):
        scratch = [pltpu.VMEM((K, K), jnp.float32)] * 2
    shapes = [jax.ShapeDtypeStruct(s, jnp.float32) for s in outs]
    return pl.pallas_call(
        kernel,
        out_shape=shapes,
        in_specs=specs,
        out_specs=[vmem] * len(outs),
        scratch_shapes=scratch,
        cost_estimate=pl.CostEstimate(flops=flops, bytes_accessed=10**6, transcendentals=0),
    )(*args)


def exchange(value, axis):
    return lax.ppermute(value, axis, [(0, 1), (1, 0)])


def body(solved, right):
    both = jnp.concatenate([solved, right], axis=0)
    count = both.shape[0]
    packed = both.reshape(count, 8, 16, 512).transpose(2, 0, 1, 3)
    rows = lax.all_to_all(packed, COLS, 0, 0, tiled=True)
    (gram,) = call(gram_kernel, [(8, LEVELS, 16, (LEVELS - 1) * K)], rows)
    gram = lax.all_to_all(gram, GROUP, 0, 0, tiled=True)
    h = gram.reshape(2, 4, LEVELS, 16, (LEVELS - 1) * K).sum(axis=1)

    slices = jnp.broadcast_to(h[:, 0], (8, 2, 16, (LEVELS - 1) * K))
    panels = lax.all_to_all(slices, GROUP, 0, 0, tiled=True)
    x0, s0 = call(level0_kernel, [(2, 5, 16, K), (5, 16, 4 * K)], panels, h)

    other = exchange(s0[1:], "yh")
    panels = lax.all_to_all(jnp.broadcast_to(s0[0], (16, 16, 4 * K)), COLS, 0, 0, tiled=True)
    side = lax.axis_index("yh").astype(jnp.int32).reshape(1)
    x1, s1 = call(level1_kernel, [(4, 16, K), (4, 16, 3 * K)], side, panels, s0, other, scalar=True)

    s1 = lax.all_to_all(jnp.broadcast_to(s1, (8, 4, 16, 3 * K)), GROUP, 0, 0, tiled=True)
    x2, s2 = call(level2_kernel, [(3 * K, K), (3 * K, 2 * K)], s1, exchange(s1, "core"))
    x3, s3 = call(level3_kernel, [(2 * K, K), (2 * K, K)], s2, exchange(s2, "z0"))
    (x4,) = call(level4_kernel, [(K, K)], s3, exchange(s3, "z1"))

    x0 = jnp.broadcast_to(x0[:, None], (2, 4, 5, 16, K)).reshape(8, 5, 16, K)
    x1 = jnp.broadcast_to(x1, (8, 4, 16, K))
    x01 = lax.all_to_all(jnp.concatenate([x0, x1], axis=1), GROUP, 0, 0, tiled=True)
    (out,) = call(finish_kernel, [(16, 5, 8, 512)], rows, x01[:, :5], x01[:, 5:], x2, x3, x4)
    out = lax.all_to_all(out, COLS, 0, 0, tiled=True)
    return out.transpose(1, 2, 0, 3).reshape(LEVELS - 1, 8, 8192)


def solution(mesh):
    fine = Mesh(np.array(mesh.devices).reshape(2, 2, 2, 2, 2, 2, 4), ROWS + COLS)
    spec = P(None, COLS, ROWS)
    return jax.shard_map(body, mesh=fine, in_specs=(spec, spec), out_specs=spec, check_vma=False)
```

```python
import jax
import jax.numpy as jnp
import numpy as np
from jax import lax
from jax.experimental import pallas as pl
from jax.experimental.pallas import tpu as pltpu
from jax.sharding import Mesh
from jax.sharding import PartitionSpec as P

ROWS = ("zt", "z1", "z0", "core")
COLS = ("yh", "yl", "x")
GROUP = ("yl", "x")
LEVELS = 6
K = 128
HIGHEST = lax.Precision.HIGHEST


def dot(a, b):
    return jnp.dot(a, b, precision=HIGHEST, preferred_element_type=jnp.float32)


def dot_t(a, b):
    return lax.dot_general(a, b, (((1,), (1,)), ((), ())), precision=HIGHEST, preferred_element_type=jnp.float32)


def inverse(coupling, x_ref, r_ref):
    rows = lax.broadcasted_iota(jnp.int32, (K, K), 0)
    cols = lax.broadcasted_iota(jnp.int32, (K, K), 1)
    eye = jnp.where(rows == cols, 1.0, 0.0).astype(jnp.float32)
    matrix = eye - coupling
    square = dot(coupling, coupling)
    quick = jnp.sum(square * square) < 0.25

    @pl.when(quick)
    def _():
        x_ref[...] = eye + coupling
        r_ref[...] = square

    @pl.when(jnp.logical_not(quick))
    def _():
        size = jnp.abs(matrix)
        scale = 1.0 / (jnp.max(jnp.sum(size, axis=0)) * jnp.max(jnp.sum(size, axis=1)))
        start = matrix.T * scale
        x_ref[...] = start
        r_ref[...] = eye - dot(start, matrix)

    def size_of(r):
        return jnp.sum(r * r)

    def going(carry):
        step, size = carry
        return jnp.logical_and(step < 80, size > 1e-6)

    def refine(carry):
        step, _ = carry
        x = x_ref[...] + dot(r_ref[...], x_ref[...])
        r = eye - dot(x, matrix)
        x_ref[...] = x
        r_ref[...] = r
        return step + 1, size_of(r)

    lax.while_loop(going, refine, (jnp.int32(0), size_of(r_ref[...])))
    x_ref[...] = x_ref[...] + dot(r_ref[...], x_ref[...])


def eliminate(panel1, panel2, rest1, rest2, x_ref, r_ref):
    p1, p2 = panel1[:, :K], panel2[:, :K]
    inverse(dot(p1, p2), x_ref, r_ref)
    q1, q2 = rest1[:, :K], rest2[:, :K]
    x1 = dot(q2 - dot(q1, p2), x_ref[...])
    x2 = q1 - dot(x1, p1)
    if panel1.shape[1] == K:
        return x1, x2, None
    state = rest1[:, K:] + rest2[:, K:] - dot(x1, panel1[:, K:]) - dot(x2, panel2[:, K:])
    return x1, x2, state


def gram_kernel(a_ref, g_ref):
    right = a_ref[:, LEVELS:]
    right = jnp.transpose(right, (1, 0, 2, 3)).reshape((LEVELS - 1) * K, -1)
    for m in range(LEVELS):
        g = dot_t(a_ref[:, m].reshape(K, -1), right)
        g_ref[:, m] = g.reshape(8, 16, (LEVELS - 1) * K)


def level0_kernel(ag_ref, h_ref, x_out, panel_out, rest_out, x_ref, r_ref):
    width = (LEVELS - 1) * K
    p1, p2 = ag_ref[:, 0].reshape(K, width), ag_ref[:, 1].reshape(K, width)
    n = LEVELS - 1
    x1, x2, state = eliminate(
        p1, p2, h_ref[0, 1:].reshape(n * 16, width), h_ref[1, 1:].reshape(n * 16, width), x_ref, r_ref
    )
    state = state.reshape(n, 16, width - K)
    panel_out[...] = jnp.broadcast_to(state[0], panel_out.shape)
    rest_out[...] = state[1:]
    x_out[0] = x1.reshape(n, 16, K)
    x_out[1] = x2.reshape(n, 16, K)


def level1_kernel(side_ref, ag_ref, own_ref, other_ref, x0_ref, x_out, s_out, x_ref, r_ref):
    width = (LEVELS - 2) * K
    n = LEVELS - 2
    side = side_ref[0]
    p1 = ag_ref[pl.ds(side * 8, 8)].reshape(K, width)
    p2 = ag_ref[pl.ds((1 - side) * 8, 8)].reshape(K, width)
    x1, _, state = eliminate(
        p1, p2, own_ref[...].reshape(n * 16, width), other_ref[...].reshape(n * 16, width), x_ref, r_ref
    )
    half = (4, n + 1, 16, K)
    x_out[:4, : n + 1] = jnp.broadcast_to(x0_ref[0], half)
    x_out[4:, : n + 1] = jnp.broadcast_to(x0_ref[1], half)
    x_out[:, n + 1 :] = jnp.broadcast_to(x1.reshape(n, 16, K), (8, n, 16, K))
    s_out[...] = jnp.broadcast_to(state.reshape(n, 16, width - K), s_out.shape)


def level2_kernel(own_ref, other_ref, x_out, s_out, x_ref, r_ref):
    width = (LEVELS - 3) * K
    n = LEVELS - 3

    def rest(ref):
        return jnp.concatenate([ref[:, m].reshape(K, width) for m in range(1, n + 1)], axis=0)

    x1, _, state = eliminate(
        own_ref[:, 0].reshape(K, width), other_ref[:, 0].reshape(K, width), rest(own_ref), rest(other_ref), x_ref, r_ref
    )
    x_out[...] = x1
    s_out[...] = state


def level3_kernel(own_ref, other_ref, x_out, s_out, x_ref, r_ref):
    x1, _, state = eliminate(own_ref[:K], other_ref[:K], own_ref[K:], other_ref[K:], x_ref, r_ref)
    x_out[...] = x1
    s_out[...] = state


def level4_kernel(own_ref, other_ref, x_out, x_ref, r_ref):
    x1, _, _ = eliminate(own_ref[:K], other_ref[:K], own_ref[K:], other_ref[K:], x_ref, r_ref)
    x_out[...] = x1


def finish_kernel(a_ref, x01_ref, x2_ref, o_ref, part_ref):
    done = [a_ref[:, 0].reshape(K, -1)]

    def factor(level, i):
        if level == 2:
            return x2_ref[i * K : (i + 1) * K]
        return x01_ref[:, (LEVELS - 1) * level + i].reshape(K, K)

    for m in range(1, LEVELS):
        value = a_ref[:, m].reshape(K, -1)
        for level in range(min(m, 3)):
            value = value - dot(factor(level, m - level - 1), done[level])
        done.append(value)
        if m < 4:
            o_ref[:, m - 1] = value.reshape(16, 8, -1)
        else:
            part_ref[:, m - 4] = value.reshape(16, 8, -1)


def later_kernel(o_ref, part_ref, x3_ref, r_ref):
    base = o_ref[:, 2].reshape(K, -1)
    for i in range(2):
        value = part_ref[:, i].reshape(K, -1) - dot(x3_ref[i * K : (i + 1) * K], base)
        r_ref[:, i] = value.reshape(16, 8, -1)


def last_kernel(part_ref, x4_ref, r_ref):
    base = part_ref[:, 0]
    value = part_ref[:, 1].reshape(K, -1) - dot(x4_ref[...], base.reshape(K, -1))
    r_ref[:, 0] = base
    r_ref[:, 1] = value.reshape(16, 8, -1)


def call(kernel, outs, *args, scalar=False, flops=10**8):
    vmem = pl.BlockSpec(memory_space=pltpu.VMEM)
    specs = [vmem] * len(args)
    if scalar:
        specs[0] = pl.BlockSpec(memory_space=pltpu.SMEM)
    scratch = []
    if kernel.__name__.startswith("level"):
        scratch = [pltpu.VMEM((K, K), jnp.float32)] * 2
    shapes = [jax.ShapeDtypeStruct(s, jnp.float32) for s in outs]
    return pl.pallas_call(
        kernel,
        out_shape=shapes,
        in_specs=specs,
        out_specs=[vmem] * len(outs),
        scratch_shapes=scratch,
        compiler_params=pltpu.CompilerParams(vmem_limit_bytes=LIMIT[kernel.__name__] << 20),
        cost_estimate=pl.CostEstimate(flops=flops, bytes_accessed=10**6, transcendentals=0),
    )(*args)


def exchange(value, axis):
    return lax.ppermute(value, axis, [(0, 1), (1, 0)])


def spread(value, axes):
    return lax.all_to_all(value, axes, 0, 0, tiled=True)


def steps(solved, right):
    both = jnp.concatenate([solved, right], axis=0)
    count = both.shape[0]
    packed = both.reshape(count, 8, 16, 512).transpose(2, 0, 1, 3)
    rows = spread(packed, COLS)
    (gram,) = call(gram_kernel, [(8, LEVELS, 16, (LEVELS - 1) * K)], rows)
    gram = spread(gram, GROUP)
    h = gram.reshape(2, 4, LEVELS, 16, (LEVELS - 1) * K).sum(axis=1)

    slices = jnp.broadcast_to(h[:, 0], (8, 2, 16, (LEVELS - 1) * K))
    panels = spread(slices, GROUP)
    x0, panel, rest = call(level0_kernel, [(2, 5, 16, K), (16, 16, 4 * K), (4, 16, 4 * K)], panels, h)

    other = exchange(rest, "yh")
    panels = spread(panel, COLS)
    side = lax.axis_index("yh").astype(jnp.int32).reshape(1)
    x01, s1 = call(level1_kernel, [(8, 9, 16, K), (8, 4, 16, 3 * K)], side, panels, rest, other, x0, scalar=True)

    s1 = spread(s1, GROUP)
    other = exchange(s1, "core")
    x01 = spread(x01, GROUP)
    x2, s2 = call(level2_kernel, [(3 * K, K), (3 * K, 2 * K)], s1, other)
    other = exchange(s2, "z0")
    early, part = call(finish_kernel, [(16, 3, 8, 512), (16, 2, 8, 512)], rows, x01, x2)
    early_out = spread(early, COLS)
    x3, s3 = call(level3_kernel, [(2 * K, K), (2 * K, K)], s2, other)
    other = exchange(s3, "z1")
    (part,) = call(later_kernel, [(16, 2, 8, 512)], early, part, x3)
    (x4,) = call(level4_kernel, [(K, K)], s3, other)
    (late,) = call(last_kernel, [(16, 2, 8, 512)], part, x4)
    late, early_out = lax.optimization_barrier((late, early_out))
    late = spread(late, COLS)
    out = jnp.concatenate([early_out, late], axis=1)
    return out.transpose(1, 2, 0, 3).reshape(LEVELS - 1, 8, 8192)


def solution(mesh):
    fine = Mesh(np.array(mesh.devices).reshape(2, 2, 2, 2, 2, 2, 4), ROWS + COLS)
    spec = P(None, COLS, ROWS)
    return jax.shard_map(steps, mesh=fine, in_specs=(spec, spec), out_specs=spec, check_vma=False)


LIMIT = dict(
    gram_kernel=24,
    level0_kernel=12,
    level1_kernel=12,
    level2_kernel=12,
    level3_kernel=12,
    level4_kernel=12,
    finish_kernel=24,
    later_kernel=12,
    last_kernel=12,
)
```

```python
import functools

import jax
import jax.numpy as jnp
import numpy as np
from jax import lax
from jax.experimental import pallas as pl
from jax.experimental.pallas import tpu as pltpu
from jax.sharding import Mesh
from jax.sharding import PartitionSpec as P

ROWS = ("zt", "z1", "z0", "core")
COLS = ("yh", "yl", "x")
GROUP = ("yl", "x")
LEVELS = 6
K = 128
HIGHEST = lax.Precision.HIGHEST


def dot(a, b):
    return jnp.dot(a, b, precision=HIGHEST, preferred_element_type=jnp.float32)


def dot_t(a, b):
    return lax.dot_general(a, b, (((1,), (1,)), ((), ())), precision=HIGHEST, preferred_element_type=jnp.float32)


def inverse(coupling, x_ref, r_ref):
    rows = lax.broadcasted_iota(jnp.int32, (K, K), 0)
    cols = lax.broadcasted_iota(jnp.int32, (K, K), 1)
    eye = jnp.where(rows == cols, 1.0, 0.0).astype(jnp.float32)
    matrix = eye - coupling
    x = eye + coupling
    x = x + dot(dot(coupling, coupling), x)
    r = eye - dot(x, matrix)
    size = jnp.sum(r * r)
    x_ref[...] = x + dot(r, x)

    @pl.when(jnp.logical_not(size < 1e-6))
    def _():
        @pl.when(jnp.logical_not(size < 0.25))
        def _():
            weight = jnp.abs(matrix)
            scale = 1.0 / (jnp.max(jnp.sum(weight, axis=0)) * jnp.max(jnp.sum(weight, axis=1)))
            x_ref[...] = matrix.T * scale

        def residual():
            r = eye - dot(x_ref[...], matrix)
            r_ref[...] = r
            return jnp.sum(r * r)

        def refine():
            x_ref[...] = x_ref[...] + dot(r_ref[...], x_ref[...])

        def going(carry):
            step, size = carry
            return jnp.logical_and(step < 80, size > 1e-6)

        def again(carry):
            step, _ = carry
            refine()
            return step + 1, residual()

        lax.while_loop(going, again, (jnp.int32(0), residual()))
        refine()


def eliminate(panel1, panel2, rest1, rest2, x_ref, r_ref):
    target = rest2[:, :K] - dot(rest1[:, :K], panel2[:, :K])
    inverse(dot(panel1[:, :K], panel2[:, :K]), x_ref, r_ref)
    return substitute(panel1, panel2, rest1, rest2, target, x_ref)


def substitute(panel1, panel2, rest1, rest2, target, x_ref):
    x1 = dot(target, x_ref[...])
    x2 = rest1[:, :K] - dot(x1, panel1[:, :K])
    if panel1.shape[1] == K:
        return x1, x2, None
    state = rest1[:, K:] + rest2[:, K:] - dot(x1, panel1[:, K:]) - dot(x2, panel2[:, K:])
    return x1, x2, state


def unpack_kernel(early_ref, late_ref, o_ref):
    for part in range(16):
        cut = slice(part * 512, (part + 1) * 512)
        o_ref[:3, :, cut] = early_ref[part]
        o_ref[3:, :, cut] = late_ref[part]


def gram_kernel(steps, ids_ref, a_ref, *g_refs):
    right = a_ref[:, LEVELS:]
    right = jnp.transpose(right, (1, 0, 2, 3)).reshape((LEVELS - 1) * K, -1)
    left = []
    for step in steps:
        member = jnp.bitwise_xor(ids_ref[0], step)
        block = a_ref[pl.ds(2 * member, 2), :LEVELS]
        left.append(jnp.transpose(block, (1, 0, 2, 3)).reshape(LEVELS * 16, -1))
    gram = dot_t(jnp.concatenate(left, axis=0), right)
    for at, g_ref in enumerate(g_refs):
        g_ref[...] = gram[at * LEVELS * 16 : (at + 1) * LEVELS * 16].reshape(LEVELS, 16, -1)


def level0_kernel(ids_ref, ag_ref, own_ref, other_ref, x_out, panel_out, rest_out, x_ref, r_ref):
    width = (LEVELS - 1) * K
    side = ids_ref[1]

    def panel(at):
        return jnp.concatenate([ag_ref[:4, at], ag_ref[4:, 1 - at]], axis=0).reshape(K, width)

    n = LEVELS - 1
    x1, x2, state = eliminate(
        panel(side),
        panel(1 - side),
        own_ref[1:].reshape(n * 16, width),
        other_ref[1:].reshape(n * 16, width),
        x_ref,
        r_ref,
    )
    state = state.reshape(n, 16, width - K)
    panel_out[...] = jnp.broadcast_to(state[0], panel_out.shape)
    rest_out[...] = state[1:]
    x_out[side] = x1.reshape(n, 16, K)
    x_out[1 - side] = x2.reshape(n, 16, K)


def level1_panels(ids_ref, ag_ref):
    width = (LEVELS - 2) * K
    side = ids_ref[2]
    p1 = ag_ref[pl.ds(side * 8, 8)].reshape(K, width)
    p2 = ag_ref[pl.ds((1 - side) * 8, 8)].reshape(K, width)
    return p1, p2


def level1_inverse_kernel(ids_ref, ag_ref, x_ref, r_ref):
    p1, p2 = level1_panels(ids_ref, ag_ref)
    inverse(dot(p1[:, :K], p2[:, :K]), x_ref, r_ref)


def level1_kernel(ids_ref, ag_ref, own_ref, other_ref, x0_ref, inverse_ref, x_out, s_out):
    width = (LEVELS - 2) * K
    n = LEVELS - 2
    p1, p2 = level1_panels(ids_ref, ag_ref)
    own, other = own_ref[...].reshape(n * 16, width), other_ref[...].reshape(n * 16, width)
    target = other[:, :K] - dot(own[:, :K], p2[:, :K])
    x1, _, state = substitute(p1, p2, own, other, target, inverse_ref)
    half = (4, n + 1, 16, K)
    x_out[:4, : n + 1] = jnp.broadcast_to(x0_ref[0], half)
    x_out[4:, : n + 1] = jnp.broadcast_to(x0_ref[1], half)
    x_out[:, n + 1 :] = jnp.broadcast_to(x1.reshape(n, 16, K), (8, n, 16, K))
    s_out[...] = jnp.broadcast_to(state.reshape(n, 16, width - K), s_out.shape)


def level2_kernel(own_ref, other_ref, x_out, s_out, x_ref, r_ref):
    width = (LEVELS - 3) * K
    n = LEVELS - 3

    def rest(ref):
        return jnp.concatenate([ref[:, m].reshape(K, width) for m in range(1, n + 1)], axis=0)

    x1, _, state = eliminate(
        own_ref[:, 0].reshape(K, width), other_ref[:, 0].reshape(K, width), rest(own_ref), rest(other_ref), x_ref, r_ref
    )
    x_out[...] = x1
    s_out[...] = state


def level3_kernel(own_ref, other_ref, x_out, s_out, x_ref, r_ref):
    x1, _, state = eliminate(own_ref[:K], other_ref[:K], own_ref[K:], other_ref[K:], x_ref, r_ref)
    x_out[...] = x1
    s_out[...] = state


def level4_kernel(own_ref, other_ref, x_out, x_ref, r_ref):
    x1, _, _ = eliminate(own_ref[:K], other_ref[:K], own_ref[K:], other_ref[K:], x_ref, r_ref)
    x_out[...] = x1


def finish_kernel(a_ref, x01_ref, x2_ref, o_ref, part_ref):
    done = [a_ref[:, 0].reshape(K, -1)]

    def factor(level, i):
        if level == 2:
            return x2_ref[i * K : (i + 1) * K]
        return x01_ref[:, (LEVELS - 1) * level + i].reshape(K, K)

    for m in range(1, LEVELS):
        value = a_ref[:, m].reshape(K, -1)
        for level in range(min(m, 3)):
            value = value - dot(factor(level, m - level - 1), done[level])
        done.append(value)
        if m < 4:
            o_ref[:, m - 1] = value.reshape(16, 8, -1)
        else:
            part_ref[:, m - 4] = value.reshape(16, 8, -1)


def later_kernel(o_ref, part_ref, x3_ref, r_ref):
    base = o_ref[:, 2].reshape(K, -1)
    for i in range(2):
        value = part_ref[:, i].reshape(K, -1) - dot(x3_ref[i * K : (i + 1) * K], base)
        r_ref[:, i] = value.reshape(16, 8, -1)


def last_kernel(part_ref, x4_ref, r_ref):
    base = part_ref[:, 0]
    value = part_ref[:, 1].reshape(K, -1) - dot(x4_ref[...], base.reshape(K, -1))
    r_ref[:, 0] = base
    r_ref[:, 1] = value.reshape(16, 8, -1)


def call(kernel, outs, *args, scalar=False, flops=10**8, name=None):
    name = name or kernel.__name__
    vmem = pl.BlockSpec(memory_space=pltpu.VMEM)
    specs = [vmem] * len(args)
    square = pltpu.VMEM((K, K), jnp.float32)
    scratch = []
    if scalar:
        specs[0] = pl.BlockSpec(memory_space=pltpu.SMEM)
    if name == "level1_inverse_kernel":
        scratch = [square]
    elif name.startswith("level") and name != "level1_kernel":
        scratch = [square] * 2
    return pl.pallas_call(
        kernel,
        out_shape=[jax.ShapeDtypeStruct(s, jnp.float32) for s in outs],
        in_specs=specs,
        out_specs=[vmem] * len(outs),
        scratch_shapes=scratch,
        compiler_params=pltpu.CompilerParams(vmem_limit_bytes=LIMIT[name] << 20),
        cost_estimate=pl.CostEstimate(flops=flops, bytes_accessed=10**6, transcendentals=0),
    )(*args)


def exchange(value, axis):
    return lax.ppermute(value, axis, [(0, 1), (1, 0)])


def reach(value, step):
    if step == 0:
        return value
    return lax.ppermute(value, GROUP, [(at, at ^ step) for at in range(8)])


def spread(value, axes):
    return lax.all_to_all(value, axes, 0, 0, tiled=True)


def steps(solved, right):
    ids = jnp.stack([lax.axis_index(GROUP), lax.axis_index("yl"), lax.axis_index("yh")]).astype(jnp.int32)
    solved, ids = lax.optimization_barrier((solved, ids))
    both = jnp.concatenate([solved, right], axis=0)
    packed = both.reshape(both.shape[0], 8, 16, 512).transpose(2, 0, 1, 3)
    rows = spread(packed, COLS)
    shape = (LEVELS, 16, (LEVELS - 1) * K)
    grams = {}
    for name, chosen in (("gram_far_kernel", (5, 6, 7, 4)), ("gram_near_kernel", (2, 1, 3, 0))):
        made = call(functools.partial(gram_kernel, chosen), [shape] * 4, ids, rows, scalar=True, flops=10**9, name=name)
        grams.update({step: reach(g, step) for step, g in zip(chosen, made)})
    own = grams[0] + grams[1] + grams[2] + grams[3]
    other = grams[4] + grams[5] + grams[6] + grams[7]

    slices = jnp.broadcast_to(jnp.stack([own[0], other[0]]), (8, 2, 16, (LEVELS - 1) * K))
    panels = spread(slices, GROUP)
    outs = [(2, 5, 16, K), (16, 16, 4 * K), (4, 16, 4 * K)]
    x0, panel, rest = call(level0_kernel, outs, ids, panels, own, other, scalar=True)

    other = exchange(rest, "yh")
    panels = spread(panel, COLS)
    (inv,) = call(level1_inverse_kernel, [(K, K)], ids, panels, scalar=True)
    outs = [(8, 9, 16, K), (8, 4, 16, 3 * K)]
    x01, s1 = call(level1_kernel, outs, ids, panels, rest, other, x0, inv, scalar=True)

    s1 = spread(s1, GROUP)
    other = exchange(s1, "core")
    x01 = spread(x01, GROUP)
    x2, s2 = call(level2_kernel, [(3 * K, K), (3 * K, 2 * K)], s1, other)
    other = exchange(s2, "z0")
    early, part = call(finish_kernel, [(16, 3, 8, 512), (16, 2, 8, 512)], rows, x01, x2)
    early_out = spread(early, COLS)
    x3, s3 = call(level3_kernel, [(2 * K, K), (2 * K, K)], s2, other)
    other = exchange(s3, "z1")
    (part,) = call(later_kernel, [(16, 2, 8, 512)], early, part, x3)
    (x4,) = call(level4_kernel, [(K, K)], s3, other)
    (late,) = call(last_kernel, [(16, 2, 8, 512)], part, x4)
    late, early_out = lax.optimization_barrier((late, early_out))
    late = spread(late, COLS)
    (out,) = call(unpack_kernel, [(LEVELS - 1, 8, 8192)], early_out, late)
    return out


def solution(mesh):
    fine = Mesh(np.array(mesh.devices).reshape(2, 2, 2, 2, 2, 2, 4), ROWS + COLS)
    spec = P(None, COLS, ROWS)
    return jax.shard_map(steps, mesh=fine, in_specs=(spec, spec), out_specs=spec, check_vma=False)


LIMIT = dict(
    unpack_kernel=12,
    gram_far_kernel=24,
    gram_near_kernel=24,
    level0_kernel=12,
    level1_inverse_kernel=12,
    level1_kernel=12,
    level2_kernel=12,
    level3_kernel=12,
    level4_kernel=12,
    finish_kernel=24,
    later_kernel=12,
    last_kernel=12,
)
```

```python
import functools

import jax
import jax.numpy as jnp
import numpy as np
from jax import lax
from jax.experimental import pallas as pl
from jax.experimental.pallas import tpu as pltpu
from jax.sharding import Mesh
from jax.sharding import PartitionSpec as P

ROWS = ("zt", "z1", "z0", "core")
COLS = ("yh", "yl", "x")
GROUP = ("yl", "x")
LEVELS = 6
K = 128
HIGHEST = lax.Precision.HIGHEST


def dot(a, b):
    return jnp.dot(a, b, precision=HIGHEST, preferred_element_type=jnp.float32)


def dot_t(a, b):
    return lax.dot_general(a, b, (((1,), (1,)), ((), ())), precision=HIGHEST, preferred_element_type=jnp.float32)


def inverse(coupling, x_ref, r_ref):
    rows = lax.broadcasted_iota(jnp.int32, (K, K), 0)
    cols = lax.broadcasted_iota(jnp.int32, (K, K), 1)
    eye = jnp.where(rows == cols, 1.0, 0.0).astype(jnp.float32)
    matrix = eye - coupling
    x = eye + coupling
    x = x + dot(dot(coupling, coupling), x)
    r = eye - dot(x, matrix)
    size = jnp.sum(r * r)
    x_ref[...] = x + dot(r, x)

    @pl.when(jnp.logical_not(size < 1e-6))
    def _():
        @pl.when(jnp.logical_not(size < 0.25))
        def _():
            weight = jnp.abs(matrix)
            scale = 1.0 / (jnp.max(jnp.sum(weight, axis=0)) * jnp.max(jnp.sum(weight, axis=1)))
            x_ref[...] = matrix.T * scale

        def residual():
            r = eye - dot(x_ref[...], matrix)
            r_ref[...] = r
            return jnp.sum(r * r)

        def refine():
            x_ref[...] = x_ref[...] + dot(r_ref[...], x_ref[...])

        def going(carry):
            step, size = carry
            return jnp.logical_and(step < 80, size > 1e-6)

        def again(carry):
            step, _ = carry
            refine()
            return step + 1, residual()

        lax.while_loop(going, again, (jnp.int32(0), residual()))
        refine()


def eliminate(panel1, panel2, rest1, rest2, x_ref, r_ref):
    target = rest2[:, :K] - dot(rest1[:, :K], panel2[:, :K])
    inverse(dot(panel1[:, :K], panel2[:, :K]), x_ref, r_ref)
    return substitute(panel1, panel2, rest1, rest2, target, x_ref)


def substitute(panel1, panel2, rest1, rest2, target, x_ref):
    x1 = dot(target, x_ref[...])
    x2 = rest1[:, :K] - dot(x1, panel1[:, :K])
    if panel1.shape[1] == K:
        return x1, x2, None
    state = rest1[:, K:] + rest2[:, K:] - dot(x1, panel1[:, K:]) - dot(x2, panel2[:, K:])
    return x1, x2, state


def unpack_kernel(early_ref, late_ref, o_ref):
    for part in range(16):
        cut = slice(part * 512, (part + 1) * 512)
        o_ref[:3, :, cut] = early_ref[part]
        o_ref[3:, :, cut] = late_ref[part]


def gram_kernel(steps, ids_ref, a_ref, *g_refs):
    right = a_ref[:, LEVELS:]
    right = jnp.transpose(right, (1, 0, 2, 3)).reshape((LEVELS - 1) * K, -1)
    left = []
    for step in steps:
        member = jnp.bitwise_xor(ids_ref[0], step)
        block = a_ref[pl.ds(2 * member, 2), :LEVELS]
        left.append(jnp.transpose(block, (1, 0, 2, 3)).reshape(LEVELS * 16, -1))
    gram = dot_t(jnp.concatenate(left, axis=0), right)
    for at, g_ref in enumerate(g_refs):
        g_ref[...] = gram[at * LEVELS * 16 : (at + 1) * LEVELS * 16].reshape(LEVELS, 16, -1)


def level0_kernel(ids_ref, ag_ref, own_ref, other_ref, x_out, panel_out, rest_out, x_ref, r_ref):
    width = (LEVELS - 1) * K
    side = ids_ref[1]

    def panel(at):
        return jnp.concatenate([ag_ref[:4, at], ag_ref[4:, 1 - at]], axis=0).reshape(K, width)

    n = LEVELS - 1
    x1, x2, state = eliminate(
        panel(side),
        panel(1 - side),
        own_ref[1:].reshape(n * 16, width),
        other_ref[1:].reshape(n * 16, width),
        x_ref,
        r_ref,
    )
    state = state.reshape(n, 16, width - K)
    panel_out[...] = jnp.broadcast_to(state[0], panel_out.shape)
    rest_out[...] = state[1:]
    x_out[side] = x1.reshape(n, 16, K)
    x_out[1 - side] = x2.reshape(n, 16, K)


def level1_panels(ids_ref, ag_ref):
    width = (LEVELS - 2) * K
    side = ids_ref[2]
    p1 = ag_ref[pl.ds(side * 8, 8)].reshape(K, width)
    p2 = ag_ref[pl.ds((1 - side) * 8, 8)].reshape(K, width)
    return p1, p2


def level1_inverse_kernel(ids_ref, ag_ref, x_ref, r_ref):
    p1, p2 = level1_panels(ids_ref, ag_ref)
    inverse(dot(p1[:, :K], p2[:, :K]), x_ref, r_ref)


def level1_kernel(ids_ref, ag_ref, own_ref, other_ref, x0_ref, inverse_ref, x_out, s_out):
    width = (LEVELS - 2) * K
    n = LEVELS - 2
    p1, p2 = level1_panels(ids_ref, ag_ref)
    own, other = own_ref[...].reshape(n * 16, width), other_ref[...].reshape(n * 16, width)
    target = other[:, :K] - dot(own[:, :K], p2[:, :K])
    x1, _, state = substitute(p1, p2, own, other, target, inverse_ref)
    half = (4, n + 1, 16, K)
    x_out[:4, : n + 1] = jnp.broadcast_to(x0_ref[0], half)
    x_out[4:, : n + 1] = jnp.broadcast_to(x0_ref[1], half)
    x_out[:, n + 1 :] = jnp.broadcast_to(x1.reshape(n, 16, K), (8, n, 16, K))
    s_out[...] = jnp.broadcast_to(state.reshape(n, 16, width - K), s_out.shape)


def level2_kernel(own_ref, other_ref, x_out, s_out, x_ref, r_ref):
    width = (LEVELS - 3) * K
    n = LEVELS - 3

    def rest(ref):
        return jnp.concatenate([ref[:, m].reshape(K, width) for m in range(1, n + 1)], axis=0)

    x1, _, state = eliminate(
        own_ref[:, 0].reshape(K, width), other_ref[:, 0].reshape(K, width), rest(own_ref), rest(other_ref), x_ref, r_ref
    )
    x_out[...] = x1
    s_out[...] = state


def level3_kernel(own_ref, other_ref, x_out, s_out, x_ref, r_ref):
    x1, _, state = eliminate(own_ref[:K], other_ref[:K], own_ref[K:], other_ref[K:], x_ref, r_ref)
    x_out[...] = x1
    s_out[...] = state


def level4_kernel(own_ref, other_ref, x_out, x_ref, r_ref):
    x1, _, _ = eliminate(own_ref[:K], other_ref[:K], own_ref[K:], other_ref[K:], x_ref, r_ref)
    x_out[...] = x1


def finish_kernel(a_ref, x01_ref, x2_ref, o_ref, part_ref):
    done = [a_ref[:, 0].reshape(K, -1)]

    def factor(level, i):
        if level == 2:
            return x2_ref[i * K : (i + 1) * K]
        return x01_ref[:, (LEVELS - 1) * level + i].reshape(K, K)

    for m in range(1, LEVELS):
        value = a_ref[:, m].reshape(K, -1)
        for level in range(min(m, 3)):
            value = value - dot(factor(level, m - level - 1), done[level])
        done.append(value)
        if m < 4:
            o_ref[:, m - 1] = value.reshape(16, 8, -1)
        else:
            part_ref[:, m - 4] = value.reshape(16, 8, -1)


def later_kernel(o_ref, part_ref, x3_ref, r_ref):
    base = o_ref[:, 2].reshape(K, -1)
    for i in range(2):
        value = part_ref[:, i].reshape(K, -1) - dot(x3_ref[i * K : (i + 1) * K], base)
        r_ref[:, i] = value.reshape(16, 8, -1)


def last_kernel(part_ref, x4_ref, r_ref):
    base = part_ref[:, 0]
    value = part_ref[:, 1].reshape(K, -1) - dot(x4_ref[...], base.reshape(K, -1))
    r_ref[:, 0] = base
    r_ref[:, 1] = value.reshape(16, 8, -1)


def call(kernel, outs, *args, scalar=False, flops=10**8, name=None):
    name = name or kernel.__name__
    vmem = pl.BlockSpec(memory_space=pltpu.VMEM)
    specs = [vmem] * len(args)
    square = pltpu.VMEM((K, K), jnp.float32)
    scratch = []
    if scalar:
        specs[0] = pl.BlockSpec(memory_space=pltpu.SMEM)
    if name == "level1_inverse_kernel":
        scratch = [square]
    elif name.startswith("level") and name != "level1_kernel":
        scratch = [square] * 2
    return pl.pallas_call(
        kernel,
        out_shape=[jax.ShapeDtypeStruct(s, jnp.float32) for s in outs],
        in_specs=specs,
        out_specs=[vmem] * len(outs),
        scratch_shapes=scratch,
        compiler_params=pltpu.CompilerParams(vmem_limit_bytes=LIMIT[name] << 20),
        cost_estimate=pl.CostEstimate(flops=flops, bytes_accessed=10**6, transcendentals=0),
    )(*args)


def exchange(value, axis):
    return lax.ppermute(value, axis, [(0, 1), (1, 0)])


def reach(value, step):
    if step == 0:
        return value
    return lax.ppermute(value, GROUP, [(at, at ^ step) for at in range(8)])


def spread(value, axes):
    return lax.all_to_all(value, axes, 0, 0, tiled=True)


def steps(solved, right):
    ids = jnp.stack([lax.axis_index(GROUP), lax.axis_index("yl"), lax.axis_index("yh")]).astype(jnp.int32)
    solved, ids = lax.optimization_barrier((solved, ids))
    both = jnp.concatenate([solved, right], axis=0)
    packed = both.reshape(both.shape[0], 8, 16, 512).transpose(2, 0, 1, 3)
    rows = spread(packed, COLS)
    shape = (LEVELS, 16, (LEVELS - 1) * K)
    grams = {}
    for name, chosen in (("gram_first_kernel", (6, 5)), ("gram_far_kernel", (7, 4)), ("gram_near_kernel", (2, 1, 3, 0))):
        made = call(functools.partial(gram_kernel, chosen), [shape] * len(chosen), ids, rows, scalar=True, flops=10**9, name=name)
        grams.update({step: reach(g, step) for step, g in zip(chosen, made)})
    own = grams[0] + grams[1] + grams[2] + grams[3]
    other = grams[4] + grams[5] + grams[6] + grams[7]

    slices = jnp.broadcast_to(jnp.stack([own[0], other[0]]), (8, 2, 16, (LEVELS - 1) * K))
    panels = spread(slices, GROUP)
    outs = [(2, 5, 16, K), (16, 16, 4 * K), (4, 16, 4 * K)]
    x0, panel, rest = call(level0_kernel, outs, ids, panels, own, other, scalar=True)

    other = exchange(rest, "yh")
    panels = spread(panel, COLS)
    (inv,) = call(level1_inverse_kernel, [(K, K)], ids, panels, scalar=True)
    outs = [(8, 9, 16, K), (8, 4, 16, 3 * K)]
    x01, s1 = call(level1_kernel, outs, ids, panels, rest, other, x0, inv, scalar=True)

    s1 = spread(s1, GROUP)
    other = exchange(s1, "core")
    x01 = spread(x01, GROUP)
    x2, s2 = call(level2_kernel, [(3 * K, K), (3 * K, 2 * K)], s1, other)
    other = exchange(s2, "z0")
    early, part = call(finish_kernel, [(16, 3, 8, 512), (16, 2, 8, 512)], rows, x01, x2)
    early_out = spread(early, COLS)
    x3, s3 = call(level3_kernel, [(2 * K, K), (2 * K, K)], s2, other)
    other = exchange(s3, "z1")
    (part,) = call(later_kernel, [(16, 2, 8, 512)], early, part, x3)
    (x4,) = call(level4_kernel, [(K, K)], s3, other)
    (late,) = call(last_kernel, [(16, 2, 8, 512)], part, x4)
    late, early_out = lax.optimization_barrier((late, early_out))
    late = spread(late, COLS)
    (out,) = call(unpack_kernel, [(LEVELS - 1, 8, 8192)], early_out, late)
    return out


def solution(mesh):
    fine = Mesh(np.array(mesh.devices).reshape(2, 2, 2, 2, 2, 2, 4), ROWS + COLS)
    spec = P(None, COLS, ROWS)
    return jax.shard_map(steps, mesh=fine, in_specs=(spec, spec), out_specs=spec, check_vma=False)


LIMIT = dict(
    unpack_kernel=12,
    gram_first_kernel=24,
    gram_far_kernel=24,
    gram_near_kernel=24,
    level0_kernel=12,
    level1_inverse_kernel=12,
    level1_kernel=12,
    level2_kernel=12,
    level3_kernel=12,
    level4_kernel=12,
    finish_kernel=58,
    later_kernel=12,
    last_kernel=12,
)
```

```python
import functools

import jax
import jax.numpy as jnp
import numpy as np
from jax import lax
from jax.experimental import pallas as pl
from jax.experimental.pallas import tpu as pltpu
from jax.sharding import Mesh
from jax.sharding import PartitionSpec as P

ROWS = ("zt", "z1", "z0", "core")
COLS = ("yh", "yl", "x")
GROUP = ("yl", "x")
LEVELS = 6
K = 128
HIGHEST = lax.Precision.HIGHEST


def dot(a, b):
    return jnp.dot(a, b, precision=HIGHEST, preferred_element_type=jnp.float32)


def dot_t(a, b):
    return lax.dot_general(a, b, (((1,), (1,)), ((), ())), precision=HIGHEST, preferred_element_type=jnp.float32)


def inverse(coupling, x_ref, r_ref):
    rows = lax.broadcasted_iota(jnp.int32, (K, K), 0)
    cols = lax.broadcasted_iota(jnp.int32, (K, K), 1)
    eye = jnp.where(rows == cols, 1.0, 0.0).astype(jnp.float32)
    matrix = eye - coupling
    x = eye + coupling
    x = x + dot(dot(coupling, coupling), x)
    r = eye - dot(x, matrix)
    size = jnp.sum(r * r)
    x_ref[...] = x + dot(r, x)

    @pl.when(jnp.logical_not(size < 1e-6))
    def _():
        @pl.when(jnp.logical_not(size < 0.25))
        def _():
            weight = jnp.abs(matrix)
            scale = 1.0 / (jnp.max(jnp.sum(weight, axis=0)) * jnp.max(jnp.sum(weight, axis=1)))
            x_ref[...] = matrix.T * scale

        def residual():
            r = eye - dot(x_ref[...], matrix)
            r_ref[...] = r
            return jnp.sum(r * r)

        def refine():
            x_ref[...] = x_ref[...] + dot(r_ref[...], x_ref[...])

        def going(carry):
            step, size = carry
            return jnp.logical_and(step < 80, size > 1e-6)

        def again(carry):
            step, _ = carry
            refine()
            return step + 1, residual()

        lax.while_loop(going, again, (jnp.int32(0), residual()))
        refine()


def eliminate(panel1, panel2, rest1, rest2, x_ref, r_ref):
    target = rest2[:, :K] - dot(rest1[:, :K], panel2[:, :K])
    inverse(dot(panel1[:, :K], panel2[:, :K]), x_ref, r_ref)
    return substitute(panel1, panel2, rest1, rest2, target, x_ref)


def substitute(panel1, panel2, rest1, rest2, target, x_ref):
    x1 = dot(target, x_ref[...])
    x2 = rest1[:, :K] - dot(x1, panel1[:, :K])
    if panel1.shape[1] == K:
        return x1, x2, None
    state = rest1[:, K:] + rest2[:, K:] - dot(x1, panel1[:, K:]) - dot(x2, panel2[:, K:])
    return x1, x2, state


def unpack_kernel(early_ref, late_ref, o_ref):
    for part in range(16):
        cut = slice(part * 512, (part + 1) * 512)
        o_ref[:3, :, cut] = early_ref[part]
        o_ref[3:, :, cut] = late_ref[part]


def gram_kernel(steps, ids_ref, a_ref, *g_refs):
    right = a_ref[:, LEVELS:]
    right = jnp.transpose(right, (1, 0, 2, 3)).reshape((LEVELS - 1) * K, -1)
    left = []
    for step in steps:
        member = jnp.bitwise_xor(ids_ref[0], step)
        block = a_ref[pl.ds(2 * member, 2), :LEVELS]
        left.append(jnp.transpose(block, (1, 0, 2, 3)).reshape(LEVELS * 16, -1))
    gram = dot_t(jnp.concatenate(left, axis=0), right)
    for at, g_ref in enumerate(g_refs):
        g_ref[...] = gram[at * LEVELS * 16 : (at + 1) * LEVELS * 16].reshape(LEVELS, 16, -1)


def level0_kernel(ids_ref, ag_ref, own_ref, other_ref, x_out, panel_out, rest_out, x_ref, r_ref):
    width = (LEVELS - 1) * K
    side = ids_ref[1]

    def panel(at):
        return jnp.concatenate([ag_ref[:4, at], ag_ref[4:, 1 - at]], axis=0).reshape(K, width)

    n = LEVELS - 1
    x1, x2, state = eliminate(
        panel(side),
        panel(1 - side),
        own_ref[1:].reshape(n * 16, width),
        other_ref[1:].reshape(n * 16, width),
        x_ref,
        r_ref,
    )
    state = state.reshape(n, 16, width - K)
    panel_out[...] = jnp.broadcast_to(state[0], panel_out.shape)
    rest_out[...] = state[1:]
    x_out[side] = x1.reshape(n, 16, K)
    x_out[1 - side] = x2.reshape(n, 16, K)


def level1_panels(ids_ref, ag_ref):
    width = (LEVELS - 2) * K
    side = ids_ref[2]
    p1 = ag_ref[pl.ds(side * 8, 8)].reshape(K, width)
    p2 = ag_ref[pl.ds((1 - side) * 8, 8)].reshape(K, width)
    return p1, p2


def level1_inverse_kernel(ids_ref, ag_ref, x_ref, r_ref):
    p1, p2 = level1_panels(ids_ref, ag_ref)
    inverse(dot(p1[:, :K], p2[:, :K]), x_ref, r_ref)


def level1_kernel(ids_ref, ag_ref, own_ref, other_ref, x0_ref, inverse_ref, s_out):
    width = (LEVELS - 2) * K
    n = LEVELS - 2
    p1, p2 = level1_panels(ids_ref, ag_ref)
    own, other = own_ref[...].reshape(n * 16, width), other_ref[...].reshape(n * 16, width)
    target = other[:, :K] - dot(own[:, :K], p2[:, :K])
    x1, _, state = substitute(p1, p2, own, other, target, inverse_ref)
    state = state.reshape(n, 16, width - K)
    for m in range(n):
        for level in range(3):
            block = state[m, :, level * K : (level + 1) * K]
            s_out[:, 3 * m + level] = jnp.broadcast_to(block, (8, 16, K))
    half = (4, n + 1, 16, K)
    s_out[:4, 12:17] = jnp.broadcast_to(x0_ref[0], half)
    s_out[4:, 12:17] = jnp.broadcast_to(x0_ref[1], half)
    s_out[:, 17:] = jnp.broadcast_to(x1.reshape(n, 16, K), (8, n, 16, K))


def level2_kernel(own_ref, other_ref, x_out, s_out, x_ref, r_ref):
    n = LEVELS - 3

    def member(ref, m):
        return jnp.concatenate([ref[:, 3 * m + level].reshape(K, K) for level in range(3)], axis=1)

    def rest(ref):
        return jnp.concatenate([member(ref, m) for m in range(1, n + 1)], axis=0)

    x1, _, state = eliminate(member(own_ref, 0), member(other_ref, 0), rest(own_ref), rest(other_ref), x_ref, r_ref)
    x_out[...] = x1
    s_out[...] = state


def level3_kernel(own_ref, other_ref, x_out, s_out, x_ref, r_ref):
    x1, _, state = eliminate(own_ref[:K], other_ref[:K], own_ref[K:], other_ref[K:], x_ref, r_ref)
    x_out[...] = x1
    s_out[...] = state


def level4_kernel(own_ref, other_ref, x_out, x_ref, r_ref):
    x1, _, _ = eliminate(own_ref[:K], other_ref[:K], own_ref[K:], other_ref[K:], x_ref, r_ref)
    x_out[...] = x1


def finish_kernel(a_ref, x01_ref, x2_ref, o_ref, part_ref):
    done = [a_ref[:, 0].reshape(K, -1)]

    def factor(level, i):
        if level == 2:
            return x2_ref[i * K : (i + 1) * K]
        return x01_ref[:, 12 + (LEVELS - 1) * level + i].reshape(K, K)

    for m in range(1, LEVELS):
        value = a_ref[:, m].reshape(K, -1)
        for level in range(min(m, 3)):
            value = value - dot(factor(level, m - level - 1), done[level])
        done.append(value)
        if m < 4:
            o_ref[:, m - 1] = value.reshape(16, 8, -1)
        else:
            part_ref[:, m - 4] = value.reshape(16, 8, -1)


def later_kernel(o_ref, part_ref, x3_ref, r_ref):
    base = o_ref[:, 2].reshape(K, -1)
    for i in range(2):
        value = part_ref[:, i].reshape(K, -1) - dot(x3_ref[i * K : (i + 1) * K], base)
        r_ref[:, i] = value.reshape(16, 8, -1)


def last_kernel(part_ref, x4_ref, r_ref):
    base = part_ref[:, 0]
    value = part_ref[:, 1].reshape(K, -1) - dot(x4_ref[...], base.reshape(K, -1))
    r_ref[:, 0] = base
    r_ref[:, 1] = value.reshape(16, 8, -1)


def call(kernel, outs, *args, scalar=False, flops=10**8, name=None):
    name = name or kernel.__name__
    vmem = pl.BlockSpec(memory_space=pltpu.VMEM)
    specs = [vmem] * len(args)
    square = pltpu.VMEM((K, K), jnp.float32)
    scratch = []
    if scalar:
        specs[0] = pl.BlockSpec(memory_space=pltpu.SMEM)
    if name == "level1_inverse_kernel":
        scratch = [square]
    elif name.startswith("level") and name != "level1_kernel":
        scratch = [square] * 2
    return pl.pallas_call(
        kernel,
        out_shape=[jax.ShapeDtypeStruct(s, jnp.float32) for s in outs],
        in_specs=specs,
        out_specs=[vmem] * len(outs),
        scratch_shapes=scratch,
        compiler_params=pltpu.CompilerParams(vmem_limit_bytes=LIMIT[name] << 20),
        cost_estimate=pl.CostEstimate(flops=flops, bytes_accessed=10**6, transcendentals=0),
    )(*args)


def exchange(value, axis):
    return lax.ppermute(value, axis, [(0, 1), (1, 0)])


def reach(value, step):
    if step == 0:
        return value
    return lax.ppermute(value, GROUP, [(at, at ^ step) for at in range(8)])


def spread(value, axes):
    return lax.all_to_all(value, axes, 0, 0, tiled=True)


def steps(solved, right):
    ids = jnp.stack([lax.axis_index(GROUP), lax.axis_index("yl"), lax.axis_index("yh")]).astype(jnp.int32)
    solved, ids = lax.optimization_barrier((solved, ids))
    both = jnp.concatenate([solved, right], axis=0)
    packed = both.reshape(both.shape[0], 8, 16, 512).transpose(2, 0, 1, 3)
    rows = spread(packed, COLS)
    shape = (LEVELS, 16, (LEVELS - 1) * K)
    grams = {}
    for name, chosen in (("gram_first_kernel", (6, 5)), ("gram_far_kernel", (7, 4)), ("gram_near_kernel", (2, 1, 3, 0))):
        made = call(functools.partial(gram_kernel, chosen), [shape] * len(chosen), ids, rows, scalar=True, flops=10**9, name=name)
        grams.update({step: reach(g, step) for step, g in zip(chosen, made)})
    own = grams[0] + grams[1] + grams[2] + grams[3]
    other = grams[4] + grams[5] + grams[6] + grams[7]

    slices = jnp.broadcast_to(jnp.stack([own[0], other[0]]), (8, 2, 16, (LEVELS - 1) * K))
    panels = spread(slices, GROUP)
    outs = [(2, 5, 16, K), (16, 16, 4 * K), (4, 16, 4 * K)]
    x0, panel, rest = call(level0_kernel, outs, ids, panels, own, other, scalar=True)

    other = exchange(rest, "yh")
    panels = spread(panel, COLS)
    (inv,) = call(level1_inverse_kernel, [(K, K)], ids, panels, scalar=True)
    (s1,) = call(level1_kernel, [(8, 21, 16, K)], ids, panels, rest, other, x0, inv, scalar=True)

    s1 = spread(s1, GROUP)
    other = exchange(s1[:, :12], "core")
    x2, s2 = call(level2_kernel, [(3 * K, K), (3 * K, 2 * K)], s1, other)
    other = exchange(s2, "z0")
    early, part = call(finish_kernel, [(16, 3, 8, 512), (16, 2, 8, 512)], rows, s1, x2)
    early_out = spread(early, COLS)
    x3, s3 = call(level3_kernel, [(2 * K, K), (2 * K, K)], s2, other)
    other = exchange(s3, "z1")
    (part,) = call(later_kernel, [(16, 2, 8, 512)], early, part, x3)
    (x4,) = call(level4_kernel, [(K, K)], s3, other)
    (late,) = call(last_kernel, [(16, 2, 8, 512)], part, x4)
    late, early_out = lax.optimization_barrier((late, early_out))
    late = spread(late, COLS)
    (out,) = call(unpack_kernel, [(LEVELS - 1, 8, 8192)], early_out, late)
    return out


def solution(mesh):
    fine = Mesh(np.array(mesh.devices).reshape(2, 2, 2, 2, 2, 2, 4), ROWS + COLS)
    spec = P(None, COLS, ROWS)
    return jax.shard_map(steps, mesh=fine, in_specs=(spec, spec), out_specs=spec, check_vma=False)


LIMIT = dict(
    unpack_kernel=12,
    gram_first_kernel=24,
    gram_far_kernel=24,
    gram_near_kernel=24,
    level0_kernel=12,
    level1_inverse_kernel=12,
    level1_kernel=12,
    level2_kernel=12,
    level3_kernel=12,
    level4_kernel=12,
    finish_kernel=24,
    later_kernel=12,
    last_kernel=12,
)
```
